32 devices in a mesh: dom: 8 (over y, x, core), feat: 4 (over z).
Axes of the slice: x: 2, y: 2, z: 4, core: 2. Of those that a mesh axis runs over, the one named last changes fastest.
Arguments:
- features: bfloat16 [512, 65536], P('feat', 'dom'), may hold values from -3 to 3
- send_blocks: int32 [8, 8, 8], P('dom'), may hold values from 0 to 63, as said below
- counts: int32 [8, 8], P('dom'), may hold values from 0 to 8, as said below
- tile_blocks: int32 [24, 512], P(None, 'dom'), may hold values from 0 to 127, as said below
- neighbours: int32 [24, 65536], P(None, 'dom'), may hold values from 0 to 127
- degree: int32 [65536], P('dom'), may hold values from 1 to 24
- epsilon: float32 [1], replicated, may hold values from -0.3 to 0.6
- w_first: bfloat16 [512, 512], replicated, may hold values from -0.25 to 0.25
- b_first: float32 [512], replicated, may hold values from -3 to 3
- w_second: bfloat16 [512, 512], replicated, may hold values from -0.25 to 0.25
- b_second: float32 [512], replicated, may hold values from -3 to 3
Outputs:
- updated: bfloat16 [65536, 512], P(('dom', 'feat'))
The draws below stay inside these ranges and needn't reach their ends.
Inputs may be any that keep to these rules, and one draw needn't show every extreme that they name: `send_blocks`: entry [q, p, s] is a row block of partition q; the entries of one pair (q, p) are distinct. counts[q, p] leading slots of send_blocks[q, p] are used; zero where q == p; in every draw some partition receives 8 blocks from every other partition. `tile_blocks`: an entry for a row block of partition p is below 64 (a row block of p) or equals 64 + q * 8 + s for a slot s of a partition q other than p.
All inputs are finite; a program needn't handle non-finite values.
Results may differ from the reference program's by a relative error of at most 0.0055.
Values may be sent and summed in bfloat16 or wider, within the bound.
No kernel may reach another device: no remote copies, remote signals or barrier semaphores. Data moves between devices by JAX's collectives and lax.ppermute only.
A program may use at most 64 MiB of HBM per device.

```python
import jax
import jax.numpy as jnp
from jax import lax

D = 512
H = 512
ROWS = 8192
BLOCK = 128
SLOTS = 8
NEIGH = 24
PARTITIONS = 8
NODES = 65536
BLOCKS = 64


def draw_send_blocks(key, part):
    key_list = jax.random.split(jax.random.fold_in(key, 11), PARTITIONS * PARTITIONS)

    def pick(single):
        return jax.random.permutation(single, BLOCKS)[:SLOTS]
    picked = jax.vmap(pick)(key_list)
    return picked.reshape(PARTITIONS, PARTITIONS, SLOTS).astype(jnp.int32)


def draw_counts(key, part):
    first, second = jax.random.split(jax.random.fold_in(key, 23))
    base = jax.random.randint(first, (PARTITIONS, PARTITIONS), 1, SLOTS + 1)
    heavy = jax.random.randint(second, (), 0, PARTITIONS)
    column = jnp.arange(PARTITIONS, dtype=jnp.int32)[None, :]
    rowpos = jnp.arange(PARTITIONS, dtype=jnp.int32)[:, None]
    base = jnp.where(column == heavy, SLOTS, base)
    base = jnp.where(column == rowpos, 0, base)
    return base.astype(jnp.int32)


def draw_tile_blocks(key, part):
    keys = jax.random.split(jax.random.fold_in(key, 37), 4)
    block_count = NODES // BLOCK
    shape = (block_count, NEIGH)
    dst_part = (jnp.arange(block_count, dtype=jnp.int32) // BLOCKS)[:, None]
    which = jax.random.randint(keys[0], shape, 0, 2)
    local = jax.random.randint(keys[1], shape, 0, BLOCKS)
    source = (dst_part + jax.random.randint(keys[2], shape, 1, PARTITIONS)) % PARTITIONS
    slot_pick = jax.random.randint(keys[3], shape, 0, SLOTS)
    remote = BLOCKS + source * SLOTS + slot_pick
    return jnp.where(which == 0, local, remote).astype(jnp.int32).T


def set_ends(entries, key, least, high):
    spot = [jax.random.randint(jax.random.fold_in(key, axis), (), 0, length) for axis, length in enumerate(entries.shape)]
    longest = entries.shape.index(max(entries.shape))
    beside = spot[:longest] + [(spot[longest] + 1) % entries.shape[longest]] + spot[longest + 1:]
    return entries.at[tuple(spot)].set(least).at[tuple(beside)].set(high)


def block_levels(rng, dims, pieces, low, largest):
    gain = 1.0
    for dim, shards_of in pieces:
        draws = jax.random.uniform(jax.random.fold_in(jax.random.fold_in(rng, 6), dim), (shards_of,), jnp.float32, low / len(pieces), largest / len(pieces))
        gain = gain * jnp.repeat(jnp.exp(draws), dims[dim] // shards_of).reshape((-1,) + (1,) * (len(dims) - 1 - dim))
    return gain


def noise(own_key, extent, spread, bound, cuts=(), kind=jnp.bfloat16):
    result = jax.random.normal(own_key, extent, jnp.float32) * spread
    if len(cuts) > 0:
        result = block_levels(own_key, extent, cuts, -0.22, 0.18) * result
    return jnp.clip(result, min=-bound, max=bound).astype(kind)


def setup_inputs(seed: int = 0) -> dict:
    streams_of = jax.random.split(jax.random.key(seed), 12)
    features = noise(streams_of[0], (D, NODES), 0.5, 3.0, ((0, 4), (1, 8)))
    send_blocks = draw_send_blocks(jax.random.fold_in(streams_of[11], 71), 0)
    counts = draw_counts(jax.random.fold_in(streams_of[11], 71), 0)
    tile_blocks = draw_tile_blocks(jax.random.fold_in(streams_of[11], 71), 0)
    neighbours = set_ends(jax.random.randint(streams_of[4], (NEIGH, NODES), 0, BLOCK), jax.random.fold_in(streams_of[4], 1), 0, BLOCK - 1).astype(jnp.int32)
    degree = set_ends(jax.random.randint(streams_of[5], (NODES,), 1, NEIGH + 1), jax.random.fold_in(streams_of[5], 1), 1, NEIGH).astype(jnp.int32)
    epsilon = jnp.clip(jax.random.uniform(streams_of[6], (1,), jnp.float32, -0.3, 0.6), -0.3, 0.6)
    w_first = noise(streams_of[7], (D, H), D ** -0.5, 0.25)
    b_first = noise(streams_of[8], (H,), 0.5, 3.0, (), jnp.float32)
    w_second = noise(streams_of[9], (H, D), H ** -0.5, 0.25)
    b_second = noise(streams_of[10], (D,), 0.5, 3.0, (), jnp.float32)
    return {"features": features, "send_blocks": send_blocks, "counts": counts, "tile_blocks": tile_blocks, "neighbours": neighbours, "degree": degree, "epsilon": epsilon, "w_first": w_first, "b_first": b_first, "w_second": w_second, "b_second": b_second}


def reference(features, send_blocks, counts, tile_blocks, neighbours, degree, epsilon, w_first, b_first, w_second, b_second):
    node_rows = features.T
    tile_rows = jnp.repeat(tile_blocks.T, BLOCK, axis=0)
    lists = (tile_rows * BLOCK + neighbours.T).astype(jnp.int32)
    row_ids = jnp.arange(NODES, dtype=jnp.int32)
    row_part = (row_ids // ROWS)[:, None]
    offset = jnp.maximum(lists - ROWS, 0)
    source = offset // (SLOTS * BLOCK)
    slot_index = (offset // BLOCK) % SLOTS
    in_block = offset % BLOCK
    block_index = send_blocks[source, row_part, slot_index]
    remote = source * ROWS + block_index * BLOCK + in_block
    is_local = lists < ROWS
    target = jnp.where(is_local, row_part * ROWS + lists, remote).astype(jnp.int32)
    live_mask = (jnp.arange(NEIGH, dtype=jnp.int32)[None, :] < degree[:, None]) & (is_local | (slot_index < counts[source, row_part]))
    weight = live_mask.astype(jnp.float32)
    block_rows = min(NODES, 4096)

    def block_sum(pair):
        gathered = node_rows[pair[0]].astype(jnp.float32)
        return jnp.einsum('rk,rkd->rd', pair[1], gathered)

    near_sum = lax.map(block_sum, (target.reshape(-1, block_rows, NEIGH), weight.reshape(-1, block_rows, NEIGH)))
    near_sum = near_sum.reshape(NODES, D)
    combined = ((1.0 + epsilon[0]) * node_rows.astype(jnp.float32) + near_sum).astype(jnp.bfloat16)
    pre_act = jnp.dot(combined, w_first, preferred_element_type=jnp.float32) + b_first
    activated = jax.nn.relu(pre_act).astype(jnp.bfloat16)
    return (jnp.dot(activated, w_second, preferred_element_type=jnp.float32) + b_second).astype(jnp.bfloat16)
```

```python
import functools

import jax
import jax.numpy as jnp
from jax import lax
from jax.experimental import pallas as pl
from jax.experimental.pallas import tpu as pltpu
from jax.sharding import PartitionSpec as P


BLOCK = 128
SUB = 8
HALVES = 2

VMEM = pl.BlockSpec(memory_space=pltpu.VMEM)
SMEM = pl.BlockSpec(memory_space=pltpu.SMEM)


def exchange_order(size):
    return sorted(range(size), key=lambda s: (-s.bit_length(), s))


def pick_kernel(pos_ref, blocks_ref, counts_ref, feat_ref, *out_refs, parts, slots, half):
    me = pos_ref[0]
    for i, shift in enumerate(range(1, parts)):
        peer = jnp.bitwise_xor(me, shift)
        count = counts_ref[peer]
        for s in range(slots):
            block = blocks_ref[peer, s]
            start = pl.multiple_of(block * BLOCK, BLOCK)
            tile = feat_ref[:, pl.ds(start, BLOCK)]
            tile = jnp.where(s < count, tile, jnp.zeros_like(tile))
            for h in range(HALVES):
                out_refs[h * (parts - 1) + i][:, s * BLOCK : (s + 1) * BLOCK] = tile[
                    h * half : (h + 1) * half
                ]


def gather_kernel(owner_ref, tiles_ref, gain_ref, near_ref, degree_ref, feat_ref, *rest, slots):
    halo_refs, out_ref, table_ref = rest[:-2], rest[-2], rest[-1]
    cols = feat_ref.shape[0]
    own = feat_ref.shape[1] // BLOCK
    width = near_ref.shape[0]
    chunk = out_ref.shape[1] // BLOCK

    @pl.loop(0, own)
    def _(b):
        start = pl.multiple_of(b * BLOCK, BLOCK)
        table_ref[b] = feat_ref[:, pl.ds(start, BLOCK)].astype(jnp.float32)

    for i, ref in enumerate(halo_refs):
        for s in range(slots):
            table_ref[own + slots + i * slots + s] = ref[:, s * BLOCK : (s + 1) * BLOCK].astype(
                jnp.float32
            )
    first = owner_ref[0] * chunk
    gain = gain_ref[0]
    groups = cols // SUB

    @pl.loop(0, chunk)
    def _(b):
        block = first + b
        lanes = pl.ds(pl.multiple_of(block * BLOCK, BLOCK), BLOCK)
        degree = jnp.broadcast_to(degree_ref[:, lanes], (SUB, BLOCK))
        self_tile = table_ref.at[block]
        sums = [gain * self_tile[g * SUB : (g + 1) * SUB] for g in range(groups)]
        for j in range(width):
            tile = table_ref.at[tiles_ref[j, block]]
            index = jnp.broadcast_to(near_ref[j : j + 1, lanes], (SUB, BLOCK))
            live = degree > j
            for g in range(groups):
                rows = tile[g * SUB : (g + 1) * SUB]
                found = jnp.take_along_axis(rows, index, axis=1, mode="promise_in_bounds")
                sums[g] = sums[g] + jnp.where(live, found, 0.0)
        place = pl.ds(pl.multiple_of(b * BLOCK, BLOCK), BLOCK)
        out_ref[:, place] = jnp.concatenate(sums, axis=0).astype(jnp.bfloat16)


def per_device(
    features,
    send_blocks,
    counts,
    tile_blocks,
    neighbours,
    degree,
    epsilon,
    w_first,
    b_first,
    w_second,
    b_second,
):
    cols, rows = features.shape
    parts = lax.axis_size("dom")
    groups = lax.axis_size("feat")
    me = lax.axis_index("dom").astype(jnp.int32)
    zed = lax.axis_index("feat").astype(jnp.int32)
    slots = send_blocks.shape[2]
    width = neighbours.shape[0]
    own = rows // BLOCK
    half = cols // HALVES
    owned = rows // groups

    picked = pl.pallas_call(
        functools.partial(pick_kernel, parts=parts, slots=slots, half=half),
        in_specs=[SMEM, SMEM, SMEM, VMEM],
        out_specs=[VMEM] * (HALVES * (parts - 1)),
        out_shape=[jax.ShapeDtypeStruct((half, slots * BLOCK), jnp.bfloat16)]
        * (HALVES * (parts - 1)),
        name="pick",
    )(me[None], send_blocks[0], counts[0], features)

    halo = []
    for h in range(HALVES):
        halo.append(
            [
                lax.ppermute(
                    picked[h * (parts - 1) + i], "dom", [(k, k ^ (i + 1)) for k in range(parts)]
                )
                for i in range(parts - 1)
            ]
        )

    remote = tile_blocks - own
    source = remote // slots
    tiles = jnp.where(
        remote < 0,
        tile_blocks,
        own + jnp.bitwise_xor(source, me) * slots + remote % slots,
    )
    gain = 1.0 + epsilon
    degree_row = degree[None, :]
    order = exchange_order(groups)
    parcels, w_rows = [], []
    for h in range(HALVES):
        feat_half = lax.slice_in_dim(features, h * half, (h + 1) * half, axis=0)
        for shift in order:
            owner = jnp.bitwise_xor(zed, shift)
            mixed = pl.pallas_call(
                functools.partial(gather_kernel, slots=slots),
                in_specs=[SMEM, SMEM, SMEM] + [VMEM] * (3 + parts - 1),
                out_specs=VMEM,
                out_shape=jax.ShapeDtypeStruct((half, owned), jnp.bfloat16),
                scratch_shapes=[pltpu.VMEM((own + slots * parts, half, BLOCK), jnp.float32)],
                name="aggregate",
            )(owner[None], tiles, gain, neighbours, degree_row, feat_half, *halo[h])
            if shift:
                mixed = lax.ppermute(mixed, "feat", [(k, k ^ shift) for k in range(groups)])
            parcels.append(mixed)
            w_rows.append(lax.dynamic_slice_in_dim(w_first, owner * cols + h * half, half, 0))
    flat = jnp.concatenate(parcels, axis=0)
    w_flat = jnp.concatenate(w_rows, axis=0)
    pre_act = (
        lax.dot_general(flat, w_flat, (((0,), (0,)), ((), ())), preferred_element_type=jnp.float32)
        + b_first
    )
    activated = jax.nn.relu(pre_act).astype(jnp.bfloat16)
    return (jnp.dot(activated, w_second, preferred_element_type=jnp.float32) + b_second).astype(
        jnp.bfloat16
    )


def solution(mesh):
    return jax.shard_map(
        per_device,
        mesh=mesh,
        in_specs=(
            P("feat", "dom"),
            P("dom", None, None),
            P("dom", None),
            P(None, "dom"),
            P(None, "dom"),
            P("dom"),
            P(),
            P(),
            P(),
            P(),
            P(),
        ),
        out_specs=P(("dom", "feat"), None),
        check_vma=False,
    )
```

```python
import functools

import jax
import jax.numpy as jnp
from jax import lax
from jax.experimental import pallas as pl
from jax.experimental.pallas import tpu as pltpu
from jax.sharding import PartitionSpec as P


BLOCK = 128
PACK = 16

VMEM = pl.BlockSpec(memory_space=pltpu.VMEM)
SMEM = pl.BlockSpec(memory_space=pltpu.SMEM)


def exchange_order(size):
    return sorted(range(size), key=lambda s: (-s.bit_length(), s))


def column_parts(cols):
    first = cols * 3 // 8 // PACK * PACK
    return (0, first), (first, cols)


def pick_kernel(pos_ref, blocks_ref, counts_ref, feat_ref, *out_refs, slots):
    me = pos_ref[0]
    for i, out_ref in enumerate(out_refs):
        peer = jnp.bitwise_xor(me, i + 1)
        count = counts_ref[peer]
        for s in range(slots):
            start = pl.multiple_of(blocks_ref[peer, s] * BLOCK, BLOCK)
            tile = feat_ref[:, pl.ds(start, BLOCK)]
            out_ref[:, s * BLOCK : (s + 1) * BLOCK] = jnp.where(
                s < count, tile, jnp.zeros_like(tile)
            )


def gather_kernel(owner_ref, tiles_ref, gain_ref, near_ref, feat_ref, *rest, slots):
    halo_refs, out_ref, table_ref = rest[:-2], rest[-2], rest[-1]
    own = feat_ref.shape[1] // BLOCK
    width = near_ref.shape[0]
    chunk = out_ref.shape[1] // BLOCK
    for b in range(own):
        table_ref[b] = feat_ref[:, b * BLOCK : (b + 1) * BLOCK]
    for i, ref in enumerate(halo_refs):
        for s in range(slots):
            table_ref[own + slots + i * slots + s] = ref[:, s * BLOCK : (s + 1) * BLOCK]
    first = owner_ref[0] * chunk
    gain = gain_ref[0]
    ids = lax.broadcasted_iota(jnp.int32, (BLOCK, BLOCK), 0).astype(jnp.float32)
    ids = ids.astype(jnp.bfloat16)
    one, zero = jnp.ones((), jnp.bfloat16), jnp.zeros((), jnp.bfloat16)
    per = next(k for k in (4, 2, 1) if chunk % k == 0)

    @pl.loop(0, chunk // per)
    def _(step):
        for k in range(per):
            b = step * per + k
            block = first + b
            lanes = pl.ds(pl.multiple_of(block * BLOCK, BLOCK), BLOCK)
            left, right = [], []
            for j in range(width):
                left.append(table_ref[tiles_ref[j, block]])
                row = jnp.broadcast_to(near_ref[j : j + 1, lanes], (PACK, BLOCK))
                row = jnp.concatenate([row.astype(jnp.bfloat16)] * (BLOCK // PACK), axis=0)
                right.append(jnp.where(row == ids, one, zero))
            near = jnp.dot(
                jnp.concatenate(left, axis=1),
                jnp.concatenate(right, axis=0),
                preferred_element_type=jnp.float32,
            )
            mixed = gain * table_ref[block].astype(jnp.float32) + near
            place = pl.ds(pl.multiple_of(b * BLOCK, BLOCK), BLOCK)
            out_ref[:, place] = mixed.astype(jnp.bfloat16)


def network_kernel(rows_ref, w_first_ref, b_first_ref, w_second_ref, b_second_ref, *rest):
    parcels, out_ref = rest[:-1], rest[-1]
    flat = jnp.concatenate([ref[...] for ref in parcels], axis=0)
    weights = jnp.concatenate(
        [
            w_first_ref[pl.ds(pl.multiple_of(rows_ref[i], PACK), ref.shape[0]), :]
            for i, ref in enumerate(parcels)
        ],
        axis=0,
    )
    pre_act = (
        lax.dot_general(flat, weights, (((0,), (0,)), ((), ())), preferred_element_type=jnp.float32)
        + b_first_ref[...]
    )
    activated = jnp.maximum(pre_act, 0.0).astype(jnp.bfloat16)
    out_ref[...] = (
        jnp.dot(activated, w_second_ref[...], preferred_element_type=jnp.float32) + b_second_ref[...]
    ).astype(jnp.bfloat16)


def per_device(
    features,
    send_blocks,
    counts,
    tile_blocks,
    neighbours,
    degree,
    epsilon,
    w_first,
    b_first,
    w_second,
    b_second,
):
    cols, rows = features.shape
    parts = lax.axis_size("dom")
    groups = lax.axis_size("feat")
    me = lax.axis_index("dom").astype(jnp.int32)
    zed = lax.axis_index("feat").astype(jnp.int32)
    slots = send_blocks.shape[2]
    width = neighbours.shape[0]
    own = rows // BLOCK
    owned = rows // groups

    halo, pieces = [], []
    for low, high in column_parts(cols):
        piece = lax.slice_in_dim(features, low, high, axis=0)
        picked = pl.pallas_call(
            functools.partial(pick_kernel, slots=slots),
            in_specs=[SMEM, SMEM, SMEM, VMEM],
            out_specs=[VMEM] * (parts - 1),
            out_shape=[jax.ShapeDtypeStruct((high - low, slots * BLOCK), jnp.bfloat16)]
            * (parts - 1),
            name="pick",
        )(me[None], send_blocks[0], counts[0], piece)
        pieces.append(piece)
        arrived = []
        for i in range(parts - 1):
            arrived.append(lax.ppermute(picked[i], "dom", [(k, k ^ (i + 1)) for k in range(parts)]))
        halo.append(arrived)

    remote = tile_blocks - own
    tiles = jnp.where(
        remote < 0,
        tile_blocks,
        own + jnp.bitwise_xor(remote // slots, me) * slots + remote % slots,
    )
    gain = 1.0 + epsilon
    entry = jnp.arange(width, dtype=jnp.int32)[:, None]
    near_rows = jnp.where(entry < degree[None, :], neighbours, -1).astype(jnp.float32)
    parcels, starts = [], []
    for h, (low, high) in enumerate(column_parts(cols)):
        piece, arrived = pieces[h], halo[h]
        for shift in exchange_order(groups):
            owner = jnp.bitwise_xor(zed, shift)
            at = owner[None]
            parcels.append(
                pl.pallas_call(
                    functools.partial(gather_kernel, slots=slots),
                    in_specs=[SMEM, SMEM, SMEM] + [VMEM] * (2 + parts - 1),
                    out_specs=VMEM,
                    out_shape=jax.ShapeDtypeStruct((high - low, owned), jnp.bfloat16),
                    scratch_shapes=[
                        pltpu.VMEM((own + slots * parts, high - low, BLOCK), jnp.bfloat16)
                    ],
                    name="aggregate",
                )(at, tiles, gain, near_rows, piece, *arrived)
            )
            starts.append(owner * cols + low)
            if shift:
                parcels[-1] = lax.ppermute(
                    parcels[-1], "feat", [(k, k ^ shift) for k in range(groups)]
                )
    step = min(owned, 256)
    hidden, wide = w_second.shape
    fixed = lambda i: (0, 0)
    return pl.pallas_call(
        network_kernel,
        grid=(owned // step,),
        in_specs=[
            SMEM,
            pl.BlockSpec(w_first.shape, fixed),
            pl.BlockSpec((1, hidden), fixed),
            pl.BlockSpec(w_second.shape, fixed),
            pl.BlockSpec((1, wide), fixed),
        ]
        + [pl.BlockSpec((p.shape[0], step), lambda i: (0, i)) for p in parcels],
        out_specs=pl.BlockSpec((step, wide), lambda i: (i, 0)),
        out_shape=jax.ShapeDtypeStruct((owned, wide), jnp.bfloat16),
        name="network",
    )(jnp.stack(starts), w_first, b_first[None, :], w_second, b_second[None, :], *parcels)


def solution(mesh):
    return jax.shard_map(
        per_device,
        mesh=mesh,
        in_specs=(
            P("feat", "dom"),
            P("dom", None, None),
            P("dom", None),
            P(None, "dom"),
            P(None, "dom"),
            P("dom"),
            P(),
            P(),
            P(),
            P(),
            P(),
        ),
        out_specs=P(("dom", "feat"), None),
        check_vma=False,
    )
```

```python
import functools

import jax
import jax.numpy as jnp
from jax import lax
from jax.experimental import pallas as pl
from jax.experimental.pallas import tpu as pltpu
from jax.sharding import PartitionSpec as P


BLOCK = 128
PACK = 16

VMEM = pl.BlockSpec(memory_space=pltpu.VMEM)
SMEM = pl.BlockSpec(memory_space=pltpu.SMEM)


def exchange_order(size):
    return sorted(range(size), key=lambda s: (-s.bit_length(), s))


def column_parts(cols):
    first = cols * 3 // 8 // PACK * PACK
    return (0, first), (first, cols)


def pick_kernel(pos_ref, blocks_ref, counts_ref, feat_ref, *out_refs, slots, low):
    me = pos_ref[0]
    for i, out_ref in enumerate(out_refs):
        peer = jnp.bitwise_xor(me, i + 1)
        count = counts_ref[peer]
        for s in range(slots):
            start = pl.multiple_of(blocks_ref[peer, s] * BLOCK, BLOCK)
            tile = feat_ref[low : low + out_ref.shape[0], pl.ds(start, BLOCK)]
            out_ref[:, s * BLOCK : (s + 1) * BLOCK] = jnp.where(
                s < count, tile, jnp.zeros_like(tile)
            )


def gather_kernel(owner_ref, tiles_ref, gain_ref, near_ref, feat_ref, *rest, slots, low):
    halo_refs, out_ref, table_ref = rest[:-2], rest[-2], rest[-1]
    own = feat_ref.shape[1] // BLOCK
    width = near_ref.shape[0]
    chunk = out_ref.shape[1] // BLOCK
    high = low + out_ref.shape[0]
    for b in range(own):
        table_ref[b] = feat_ref[low:high, b * BLOCK : (b + 1) * BLOCK]
    for i, ref in enumerate(halo_refs):
        for s in range(slots):
            table_ref[own + slots + i * slots + s] = ref[:, s * BLOCK : (s + 1) * BLOCK]
    first = owner_ref[0] * chunk
    gain = gain_ref[0]
    ids = lax.broadcasted_iota(jnp.int32, (BLOCK, BLOCK), 0).astype(jnp.float32)
    ids = ids.astype(jnp.bfloat16)
    one, zero = jnp.ones((), jnp.bfloat16), jnp.zeros((), jnp.bfloat16)
    per = next(k for k in (4, 2, 1) if chunk % k == 0)

    @pl.loop(0, chunk // per)
    def _(step):
        for k in range(per):
            b = step * per + k
            block = first + b
            lanes = pl.ds(pl.multiple_of(block * BLOCK, BLOCK), BLOCK)
            left, right = [], []
            for j in range(width):
                left.append(table_ref[tiles_ref[j, block]])
                row = jnp.broadcast_to(near_ref[j : j + 1, lanes], (PACK, BLOCK))
                row = jnp.concatenate([row.astype(jnp.bfloat16)] * (BLOCK // PACK), axis=0)
                right.append(jnp.where(row == ids, one, zero))
            near = jnp.dot(
                jnp.concatenate(left, axis=1),
                jnp.concatenate(right, axis=0),
                preferred_element_type=jnp.float32,
            )
            mixed = gain * table_ref[block].astype(jnp.float32) + near
            place = pl.ds(pl.multiple_of(b * BLOCK, BLOCK), BLOCK)
            out_ref[:, place] = mixed.astype(jnp.bfloat16)


def network_kernel(rows_ref, w_first_ref, b_first_ref, w_second_ref, b_second_ref, *rest):
    parcels, out_ref = rest[:-1], rest[-1]
    flat = jnp.concatenate([ref[...] for ref in parcels], axis=0)
    weights = jnp.concatenate(
        [
            w_first_ref[pl.ds(pl.multiple_of(rows_ref[i], PACK), ref.shape[0]), :]
            for i, ref in enumerate(parcels)
        ],
        axis=0,
    )
    pre_act = (
        lax.dot_general(flat, weights, (((0,), (0,)), ((), ())), preferred_element_type=jnp.float32)
        + b_first_ref[...]
    )
    activated = jnp.maximum(pre_act, 0.0).astype(jnp.bfloat16)
    out_ref[...] = (
        jnp.dot(activated, w_second_ref[...], preferred_element_type=jnp.float32) + b_second_ref[...]
    ).astype(jnp.bfloat16)


def per_device(
    features,
    send_blocks,
    counts,
    tile_blocks,
    neighbours,
    degree,
    epsilon,
    w_first,
    b_first,
    w_second,
    b_second,
):
    cols, rows = features.shape
    parts = lax.axis_size("dom")
    groups = lax.axis_size("feat")
    me = lax.axis_index("dom").astype(jnp.int32)
    zed = lax.axis_index("feat").astype(jnp.int32)
    slots = send_blocks.shape[2]
    width = neighbours.shape[0]
    own = rows // BLOCK
    owned = rows // groups

    halo = []
    for low, high in column_parts(cols):
        picked = pl.pallas_call(
            functools.partial(pick_kernel, slots=slots, low=low),
            in_specs=[SMEM, SMEM, SMEM, VMEM],
            out_specs=[VMEM] * (parts - 1),
            out_shape=[jax.ShapeDtypeStruct((high - low, slots * BLOCK), jnp.bfloat16)]
            * (parts - 1),
            name="pick",
        )(me[None], send_blocks[0], counts[0], features)
        arrived = []
        for i in range(parts - 1):
            arrived.append(lax.ppermute(picked[i], "dom", [(k, k ^ (i + 1)) for k in range(parts)]))
        halo.append(arrived)

    remote = tile_blocks - own
    tiles = jnp.where(
        remote < 0,
        tile_blocks,
        own + jnp.bitwise_xor(remote // slots, me) * slots + remote % slots,
    )
    gain = 1.0 + epsilon
    entry = jnp.arange(width, dtype=jnp.int32)[:, None]
    near_rows = jnp.where(entry < degree[None, :], neighbours, -1).astype(jnp.float32)
    parcels, starts = [], []
    for h, (low, high) in enumerate(column_parts(cols)):
        arrived = halo[h]
        for shift in exchange_order(groups):
            owner = jnp.bitwise_xor(zed, shift)
            at = owner[None]
            parcels.append(
                pl.pallas_call(
                    functools.partial(gather_kernel, slots=slots, low=low),
                    in_specs=[SMEM, SMEM, SMEM] + [VMEM] * (2 + parts - 1),
                    out_specs=VMEM,
                    out_shape=jax.ShapeDtypeStruct((high - low, owned), jnp.bfloat16),
                    scratch_shapes=[
                        pltpu.VMEM((own + slots * parts, high - low, BLOCK), jnp.bfloat16)
                    ],
                    name="aggregate",
                )(at, tiles, gain, near_rows, features, *arrived)
            )
            starts.append(owner * cols + low)
            if shift:
                parcels[-1] = lax.ppermute(
                    parcels[-1], "feat", [(k, k ^ shift) for k in range(groups)]
                )
    step = min(owned, 256)
    hidden, wide = w_second.shape
    fixed = lambda i: (0, 0)
    return pl.pallas_call(
        network_kernel,
        grid=(owned // step,),
        in_specs=[
            SMEM,
            pl.BlockSpec(w_first.shape, fixed),
            pl.BlockSpec((1, hidden), fixed),
            pl.BlockSpec(w_second.shape, fixed),
            pl.BlockSpec((1, wide), fixed),
        ]
        + [pl.BlockSpec((p.shape[0], step), lambda i: (0, i)) for p in parcels],
        out_specs=pl.BlockSpec((step, wide), lambda i: (i, 0)),
        out_shape=jax.ShapeDtypeStruct((owned, wide), jnp.bfloat16),
        name="network",
    )(jnp.stack(starts), w_first, b_first[None, :], w_second, b_second[None, :], *parcels)


def solution(mesh):
    return jax.shard_map(
        per_device,
        mesh=mesh,
        in_specs=(
            P("feat", "dom"),
            P("dom", None, None),
            P("dom", None),
            P(None, "dom"),
            P(None, "dom"),
            P("dom"),
            P(),
            P(),
            P(),
            P(),
            P(),
        ),
        out_specs=P(("dom", "feat"), None),
        check_vma=False,
    )
```
